32 devices in a mesh: gx: 4 (over z), gy: 2 (over core), gz: 4 (over y, x).
Axes of the slice: x: 2, y: 2, z: 4, core: 2. Of those that a mesh axis runs over, the one named last changes fastest.
Arguments:
- pair: bfloat16 [128, 512, 512], P('gz', 'gx', 'gy'), may hold values from -6 to 6
- pair_mask: int32 [512, 512], P('gx', 'gy'), may hold values from 0 to 1, as said below
- input_gain: float32 [128], replicated, may hold values from 0.1 to 1.9
- input_weights: bfloat16 [4, 128, 128], replicated, may hold values from -0.5 to 0.5
- out_gate_weight: bfloat16 [128, 128], replicated, may hold values from -0.5 to 0.5
- hidden_gain: float32 [128], replicated, may hold values from 0.1 to 1.9
- out_weight: bfloat16 [128, 128], replicated, may hold values from -0.5 to 0.5
Outputs:
- update: bfloat16 [128, 512, 512], P('gz', 'gx', 'gy')
The draws below stay inside these ranges and needn't reach their ends.
Inputs may be any that keep to these rules, and one draw needn't show every extreme that they name: pair_mask[r, s] = m[r] * m[s] for a 0/1 residue mask m of the draw that is 0 for all r >= L, for one crop length L with 256 < L <= 512; residues below L may also be 0.
All inputs are finite; a program needn't handle non-finite values.
Results may differ from the reference program's by a relative error of at most 0.011.
Values may be sent and summed in bfloat16 or wider, within the bound.
A program may use at most 64 MiB of HBM per device.

```python
import jax
import jax.numpy as jnp
from jax import lax

C = 128
CH = 128
N = 512


def draw_pair_mask(key, part):
    crop_length = jax.random.randint(jax.random.fold_in(key, 7), (), N // 2 + 1, N + 1)
    dropped = jax.random.randint(jax.random.fold_in(key, 11), (N,), 0, 16)
    inside = ((jnp.arange(N) < crop_length) & (dropped != 0)).astype(jnp.int32)
    return inside[:, None] * inside[None, :]


def levels(own_key, extent, split, least, largest):
    loudness, own = 1.0, jax.random.fold_in(own_key, 6)
    for axis_at, shards_of in split:
        steps = jnp.exp(jax.random.uniform(jax.random.fold_in(own, axis_at), (shards_of,), jnp.float32, least / len(split), largest / len(split)))
        loudness = loudness * jnp.repeat(steps, extent[axis_at] // shards_of).reshape([-1 if axis == axis_at else 1 for axis in range(len(extent))])
    return loudness


def bell_draw(stream_key, shape, width, most, cuts=(), kind=jnp.bfloat16):
    factor_of = levels(stream_key, shape, cuts, -0.22, 0.18) if cuts else 1.0
    result = jax.random.normal(stream_key, shape, jnp.float32) * width * factor_of
    return jnp.minimum(jnp.maximum(result, -most), most).astype(kind)


def setup_inputs(seed: int = 0) -> dict:
    seeds = jax.random.split(jax.random.key(seed), 8)
    pair = bell_draw(seeds[0], (C, N, N), 1.0, 6.0, ((0, 4), (1, 4), (2, 2)))
    pair_mask = draw_pair_mask(jax.random.fold_in(seeds[7], 71), 0)
    input_gain = jnp.clip(1.0 + 0.18 * jax.random.normal(seeds[2], (C,), jnp.float32), 0.1, 1.9)
    input_weights = bell_draw(seeds[3], (4, C, CH), C ** -0.5, 0.5)
    out_gate_weight = bell_draw(seeds[4], (C, C), C ** -0.5, 0.5)
    hidden_gain = jnp.clip(1.0 + 0.18 * jax.random.normal(seeds[5], (CH,), jnp.float32), 0.1, 1.9)
    out_weight = bell_draw(seeds[6], (CH, C), CH ** -0.5, 0.5)
    return dict(pair=pair, pair_mask=pair_mask, input_gain=input_gain, input_weights=input_weights, out_gate_weight=out_gate_weight, hidden_gain=hidden_gain, out_weight=out_weight)


EPSILON = 1e-05

def layer_norm(values, gains):
    average = lax.optimization_barrier(jnp.mean(values, axis=0))
    spread = lax.optimization_barrier(jnp.mean(jnp.square(values - average), axis=0))
    return (values - average) * lax.rsqrt(spread + EPSILON) * gains[:, None, None]

def project(weights, normed):
    return jnp.einsum('dk,drs->krs', weights.astype(jnp.float32), normed.astype(jnp.float32))

def reference(pair, pair_mask, input_gain, input_weights, out_gate_weight, hidden_gain, out_weight):
    normed = layer_norm(pair.astype(jnp.float32), input_gain).astype(jnp.bfloat16)
    mask_values = pair_mask.astype(jnp.float32)
    left_side = (mask_values * jax.nn.sigmoid(project(input_weights[0], normed)) * project(input_weights[1], normed)).astype(jnp.bfloat16)
    right_side = (mask_values * jax.nn.sigmoid(project(input_weights[2], normed)) * project(input_weights[3], normed)).astype(jnp.bfloat16)
    gate = jax.nn.sigmoid(project(out_gate_weight, normed))
    triangle = jnp.einsum('hki,hkj->hij', left_side.astype(jnp.float32), right_side.astype(jnp.float32))
    hidden_normed = layer_norm(triangle, hidden_gain).astype(jnp.bfloat16)
    projected = project(out_weight, hidden_normed)
    return (mask_values * gate * projected).astype(jnp.bfloat16)
```

```python
import functools

import jax
import jax.numpy as jnp
from jax import lax
from jax.experimental import pallas as pl
from jax.experimental.pallas import tpu as pltpu
from jax.sharding import PartitionSpec as P

EPSILON = 1e-05
MESH = pl.DeviceIdType.MESH


def position(axes):
    at = 0
    for name in axes:
        at = at * lax.axis_size(name) + lax.axis_index(name)
    return at


def coordinates(axes, at):
    where = {}
    for name in reversed(axes):
        where[name] = lax.rem(at, lax.axis_size(name))
        at = at // lax.axis_size(name)
    return where


def block(ref, axis, at, width):
    cut = [slice(None)] * len(ref.shape)
    cut[axis] = pl.ds(pl.multiple_of(at * width, width), width)
    return ref.at[tuple(cut)]


def greet(axes, others):
    me = position(axes)
    barrier = pltpu.get_barrier_semaphore()

    @pl.loop(1, others + 1)
    def _(step):
        there = coordinates(axes, lax.rem(me + step, others + 1))
        pl.semaphore_signal(barrier, inc=1, device_id=there, device_id_type=MESH)

    pl.semaphore_wait(barrier, others)


def exchange_kernel(axes, split, concat, count, src, dst, held, sends, receives, own):
    me = position(axes)
    wide = src.shape[split] // count
    tall = src.shape[concat]
    greet(axes, count - 1)

    def copy(step, sender, target):
        return pltpu.make_async_remote_copy(
            src_ref=block(src, split, target, wide),
            dst_ref=block(dst, concat, sender, tall),
            send_sem=sends.at[step],
            recv_sem=receives.at[step],
            device_id=coordinates(axes, target),
            device_id_type=MESH,
        )

    @pl.loop(1, count)
    def _(step):
        copy(step, me, lax.rem(me + step, count)).start()

    inward = pltpu.make_async_copy(block(src, split, me, wide), held, own)
    inward.start()
    inward.wait()
    outward = pltpu.make_async_copy(held, block(dst, concat, me, tall), own)
    outward.start()
    outward.wait()

    @pl.loop(1, count)
    def _(step):
        copy(step, lax.rem(me - step + count, count), lax.rem(me + step, count)).wait()


def exchange(value, axes, split, concat, number):
    count = 1
    for name in axes:
        count = count * lax.axis_size(name)
    shape = list(value.shape)
    shape[split] //= count
    piece = tuple(shape)
    shape[concat] *= count
    return pl.pallas_call(
        functools.partial(exchange_kernel, axes, split, concat, count),
        out_shape=jax.ShapeDtypeStruct(tuple(shape), value.dtype),
        in_specs=[pl.BlockSpec(memory_space=pl.ANY)],
        out_specs=pl.BlockSpec(memory_space=pl.ANY),
        scratch_shapes=[
            pltpu.VMEM(piece, value.dtype),
            pltpu.SemaphoreType.DMA((count,)),
            pltpu.SemaphoreType.DMA((count,)),
            pltpu.SemaphoreType.DMA,
        ],
        compiler_params=pltpu.CompilerParams(collective_id=number, has_side_effects=True),
    )(value)


def pair_exchange_kernel(axes, count, left, right, wide_left, far_right, held, sends, receives, gsend, greceive, own):
    me = position(axes)
    core = lax.axis_index("gy")
    cores = lax.axis_size("gy")
    hidden, tall, span = left.shape
    depth = hidden // count
    barrier = pltpu.get_barrier_semaphore()

    @pl.loop(1, count)
    def _(step):
        there = coordinates(axes, lax.rem(me + step, count))
        pl.semaphore_signal(barrier, inc=1, device_id=there, device_id_type=MESH)

    for ahead in range(1, cores):
        pl.semaphore_signal(
            barrier, inc=1, device_id={"gy": lax.rem(core + ahead, cores)}, device_id_type=MESH
        )
    pl.semaphore_wait(barrier, count - 1 + cores - 1)
    columns = pl.ds(pl.multiple_of(core * span, span), span)

    def landing(side, sender):
        rows = pl.ds(pl.multiple_of(sender * tall, tall), tall)
        return wide_left.at[:, rows, columns] if side == 0 else far_right.at[:, rows, :]

    def copy(side, step, sender, target):
        return pltpu.make_async_remote_copy(
            src_ref=block((left, right)[side], 0, target, depth),
            dst_ref=landing(side, sender),
            send_sem=sends.at[side, step],
            recv_sem=receives.at[side, step],
            device_id=coordinates(axes, target),
            device_id_type=MESH,
        )

    for side in range(2):
        @pl.loop(1, count)
        def _(step):
            copy(side, step, me, lax.rem(me + step, count)).start()

    for side in range(2):
        inward = pltpu.make_async_copy(block((left, right)[side], 0, me, depth), held, own)
        inward.start()
        inward.wait()
        outward = pltpu.make_async_copy(held, landing(side, me), own)
        outward.start()
        outward.wait()

    @pl.loop(1, count)
    def _(step):
        copy(0, step, lax.rem(me - step + count, count), lax.rem(me + step, count)).wait()

    passes = [
        pltpu.make_async_remote_copy(
            src_ref=wide_left.at[:, :, columns],
            dst_ref=wide_left.at[:, :, columns],
            send_sem=gsend.at[ahead],
            recv_sem=greceive.at[ahead],
            device_id={"gy": lax.rem(core + ahead, cores)},
            device_id_type=MESH,
        )
        for ahead in range(1, cores)
    ]
    for one in passes:
        one.start()

    @pl.loop(1, count)
    def _(step):
        copy(1, step, lax.rem(me - step + count, count), lax.rem(me + step, count)).wait()

    for one in passes:
        one.wait()


def pair_exchange(left, right, axes, number):
    count = 1
    for name in axes:
        count = count * lax.axis_size(name)
    cores = lax.axis_size("gy")
    hidden, tall, span = left.shape
    depth = hidden // count
    return pl.pallas_call(
        functools.partial(pair_exchange_kernel, axes, count),
        out_shape=(
            jax.ShapeDtypeStruct((depth, tall * count, span * cores), left.dtype),
            jax.ShapeDtypeStruct((depth, tall * count, span), left.dtype),
        ),
        in_specs=[pl.BlockSpec(memory_space=pl.ANY)] * 2,
        out_specs=(pl.BlockSpec(memory_space=pl.ANY),) * 2,
        scratch_shapes=[
            pltpu.VMEM((depth, tall, span), left.dtype),
            pltpu.SemaphoreType.DMA((2, count)),
            pltpu.SemaphoreType.DMA((2, count)),
            pltpu.SemaphoreType.DMA((cores,)),
            pltpu.SemaphoreType.DMA((cores,)),
            pltpu.SemaphoreType.DMA,
        ],
        compiler_params=pltpu.CompilerParams(collective_id=number, has_side_effects=True),
    )(left, right)


def layer_norm(values, gains):
    average = jnp.mean(values, axis=0)
    spread = jnp.mean(jnp.square(values - average), axis=0)
    return ((values - average) * lax.rsqrt(spread + EPSILON) * gains[:, None, None]).astype(jnp.bfloat16)


def project(weights, normed):
    return jnp.einsum("dk,drs->krs", weights, normed, preferred_element_type=jnp.float32)


def shards(pair, pair_mask, input_gain, input_weights, out_gate_weight, hidden_gain, out_weight):
    flat = ("gx", "gz")
    rows = pair.shape[1] // lax.axis_size("gz")
    own_mask = lax.dynamic_slice_in_dim(pair_mask, lax.axis_index("gz") * rows, rows, 0)
    mask_values = own_mask.astype(jnp.float32)
    every_channel = exchange(pair, ("gz",), 1, 0, 0)
    normed = layer_norm(every_channel.astype(jnp.float32), input_gain)
    left, right = (
        (
            mask_values
            * jax.nn.sigmoid(project(input_weights[at], normed))
            * project(input_weights[at + 1], normed)
        ).astype(jnp.bfloat16)
        for at in (0, 2)
    )
    gate = jax.nn.sigmoid(project(out_gate_weight, normed))
    wide_left, far_right = pair_exchange(left, right, flat, 1)
    triangle = jnp.einsum(
        "hki,hkj->hij", wide_left, far_right, preferred_element_type=jnp.float32
    ).astype(jnp.bfloat16)
    every_hidden = exchange(triangle, flat, 1, 0, 2)
    hidden_normed = layer_norm(every_hidden.astype(jnp.float32), hidden_gain)
    projected = project(out_weight, hidden_normed)
    update = (mask_values * gate * projected).astype(jnp.bfloat16)
    return exchange(update, ("gz",), 0, 1, 3)


def solution(mesh):
    placed = (P("gz", "gx", "gy"), P("gx", "gy"), P(), P(), P(), P(), P())
    return jax.shard_map(
        shards, mesh=mesh, in_specs=placed, out_specs=P("gz", "gx", "gy"), check_vma=False
    )
```

```python
import functools

import jax
import jax.numpy as jnp
from jax import lax
from jax.experimental import pallas as pl
from jax.experimental.pallas import tpu as pltpu
from jax.sharding import PartitionSpec as P

EPSILON = 1e-05
MESH = pl.DeviceIdType.MESH


def position(axes):
    at = 0
    for name in axes:
        at = at * lax.axis_size(name) + lax.axis_index(name)
    return at


def coordinates(axes, at):
    where = {}
    for name in reversed(axes):
        where[name] = lax.rem(at, lax.axis_size(name))
        at = at // lax.axis_size(name)
    return where


ROWS = 8
LANES = 128


def panels(span):
    return [(at, slice(at * LANES, (at + 1) * LANES)) for at in range(span // LANES)]


def row_of(store, row, height, span):
    parts = [store[at, pl.ds(row, height, stride=ROWS), :] for at, _ in panels(span)]
    return jnp.concatenate(parts, axis=1)


def put_row(store, row, height, span, value):
    for at, lanes in panels(span):
        store[at, pl.ds(row, height, stride=ROWS), :] = value[:, lanes]


def pack(store, target, span):
    for at, lanes in panels(span):
        height = store.shape[1] // ROWS
        target[:, :, lanes] = store[at].reshape(height, ROWS, LANES).astype(jnp.bfloat16)


def greet(groups):
    barrier = pltpu.get_barrier_semaphore()
    total = 0
    for axes, count in groups:
        me = position(axes)

        @pl.loop(1, count)
        def _(step):
            there = coordinates(axes, lax.rem(me + step, count))
            pl.semaphore_signal(barrier, inc=1, device_id=there, device_id_type=MESH)

        total += count - 1
    pl.semaphore_wait(barrier, total)


def standardize(source, plain):
    values = source.astype(jnp.float32)
    average = jnp.sum(values, axis=0) / values.shape[0]
    centred = values - average
    spread = jnp.sum(centred * centred, axis=0) / values.shape[0]
    result = centred * lax.rsqrt(spread + EPSILON)
    for at, lanes in panels(values.shape[2]):
        plain[at] = result[:, :, lanes].reshape(plain.shape[1:])


def front_kernel(
    flat, count, quads, pair, mask, gain, weights,
    wide_left, far_right, gate,
    landed, plain, sided, outgoing,
    pair_send, pair_recv, pair_own, sends, receives, gsend, greceive, own,
):
    me = position(flat)
    quad = lax.axis_index("gz")
    core = lax.axis_index("gy")
    cores = lax.axis_size("gy")
    chunks, channels, _, span = landed.shape
    local = pair.shape[0]
    rows = chunks * ROWS
    hidden = outgoing.shape[2]
    depth = hidden // count
    greet(((flat, count), (("gy",), cores)))
    columns = pl.ds(pl.multiple_of(core * span, span), span)

    def pair_copy(chunk, step, sender, target):
        first = pl.multiple_of(target * rows + chunk * ROWS, ROWS)
        return pltpu.make_async_remote_copy(
            src_ref=pair.at[:, pl.ds(first, ROWS), :],
            dst_ref=landed.at[chunk, pl.ds(sender * local, local)],
            send_sem=pair_send.at[chunk, step],
            recv_sem=pair_recv.at[chunk, step],
            device_id={"gz": target},
            device_id_type=MESH,
        )

    def pair_keep(chunk):
        first = pl.multiple_of(quad * rows + chunk * ROWS, ROWS)
        return pltpu.make_async_copy(
            pair.at[:, pl.ds(first, ROWS), :],
            landed.at[chunk, pl.ds(quad * local, local)],
            pair_own.at[chunk],
        )

    def landing(side, chunk, sender):
        cut = pl.ds(pl.multiple_of(chunk * ROWS, ROWS), ROWS)
        if side == 0:
            return wide_left.at[:, sender, cut, columns]
        return far_right.at[:, sender, cut, :]

    def copy(side, chunk, step, sender, target):
        return pltpu.make_async_remote_copy(
            src_ref=outgoing.at[side, chunk, pl.ds(target * depth, depth)],
            dst_ref=landing(side, chunk, sender),
            send_sem=sends.at[side, chunk, step],
            recv_sem=receives.at[side, chunk, step],
            device_id=coordinates(flat, target),
            device_id_type=MESH,
        )

    def keep(side, chunk):
        return pltpu.make_async_copy(
            outgoing.at[side, chunk, pl.ds(me * depth, depth)],
            landing(side, chunk, me),
            own.at[side, chunk],
        )

    def passed(chunk, ahead):
        cut = pl.ds(pl.multiple_of(chunk * ROWS, ROWS), ROWS)
        return pltpu.make_async_remote_copy(
            src_ref=wide_left.at[:, :, cut, columns],
            dst_ref=wide_left.at[:, :, cut, columns],
            send_sem=gsend.at[chunk, ahead],
            recv_sem=greceive.at[chunk, ahead],
            device_id={"gy": lax.rem(core + ahead, cores)},
            device_id_type=MESH,
        )

    @pl.loop(0, chunks)
    def _(chunk):
        pair_keep(chunk).start()

        @pl.loop(1, quads)
        def _(step):
            pair_copy(chunk, step, quad, lax.rem(quad + step, quads)).start()

    @pl.loop(0, chunks)
    def _(chunk):
        @pl.loop(1, quads)
        def _(step):
            pair_copy(
                chunk, step, lax.rem(quad - step + quads, quads), lax.rem(quad + step, quads)
            ).wait()

        pair_keep(chunk).wait()
        standardize(landed[chunk], plain)

        @pl.loop(0, ROWS)
        def _(row):
            normed = (row_of(plain, row, channels, span) * gain[...]).astype(jnp.bfloat16)
            inside = mask[pl.ds(chunk * ROWS + row, 1), :]

            def product(at):
                return jnp.dot(weights[at], normed, preferred_element_type=jnp.float32)

            for side in range(2):
                gated = inside * jax.nn.sigmoid(product(2 * side)) * product(2 * side + 1)
                put_row(sided.at[side], row, hidden, span, gated)
            gate[chunk * ROWS + row] = jax.nn.sigmoid(product(4))

        for side in range(2):
            pack(sided.at[side], outgoing.at[side, chunk], span)

        for side in range(2):
            @pl.loop(1, count)
            def _(step):
                copy(side, chunk, step, me, lax.rem(me + step, count)).start()

            keep(side, chunk).start()

    @pl.loop(0, chunks)
    def _(chunk):
        for side in range(2):
            @pl.loop(1, count)
            def _(step):
                copy(
                    side, chunk, step, lax.rem(me - step + count, count), lax.rem(me + step, count)
                ).wait()

            keep(side, chunk).wait()
            if side == 0:
                for ahead in range(1, cores):
                    passed(chunk, ahead).start()

    @pl.loop(0, chunks)
    def _(chunk):
        for ahead in range(1, cores):
            passed(chunk, ahead).wait()


def back_kernel(
    flat, count, quads, wide_left, far_right, gate, mask, gain, weights,
    update,
    triangle, landed, plain, sided, outgoing,
    sends, receives, out_send, out_recv, out_own,
):
    me = position(flat)
    quad = lax.axis_index("gz")
    chunks, hidden, _, span = landed.shape
    channels = outgoing.shape[1]
    local = channels // quads
    rows = chunks * ROWS
    depth = hidden // count
    greet(((flat, count),))

    def copy(chunk, step, sender, target):
        return pltpu.make_async_remote_copy(
            src_ref=triangle.at[:, target, chunk],
            dst_ref=landed.at[chunk, pl.ds(sender * depth, depth)],
            send_sem=sends.at[chunk, step],
            recv_sem=receives.at[chunk, step],
            device_id=coordinates(flat, target),
            device_id_type=MESH,
        )

    def out_copy(chunk, step, sender, target):
        first = pl.multiple_of(sender * rows + chunk * ROWS, ROWS)
        return pltpu.make_async_remote_copy(
            src_ref=outgoing.at[chunk, pl.ds(target * local, local)],
            dst_ref=update.at[:, pl.ds(first, ROWS), :],
            send_sem=out_send.at[chunk, step],
            recv_sem=out_recv.at[chunk, step],
            device_id={"gz": target},
            device_id_type=MESH,
        )

    def out_keep(chunk):
        first = pl.multiple_of(quad * rows + chunk * ROWS, ROWS)
        return pltpu.make_async_copy(
            outgoing.at[chunk, pl.ds(quad * local, local)],
            update.at[:, pl.ds(first, ROWS), :],
            out_own.at[chunk],
        )

    @pl.loop(0, depth)
    def _(at):
        product = lax.dot_general(
            wide_left[at], far_right[at], (((0,), (0,)), ((), ())),
            preferred_element_type=jnp.float32,
        )
        triangle[at] = product.reshape(count, chunks, ROWS, span).astype(jnp.bfloat16)

    @pl.loop(0, chunks)
    def _(chunk):
        @pl.loop(1, count)
        def _(step):
            copy(chunk, step, me, lax.rem(me + step, count)).start()

    @pl.loop(0, chunks)
    def _(chunk):
        @pl.loop(0, depth)
        def _(at):
            landed[chunk, me * depth + at] = triangle[at, me, chunk]

        @pl.loop(1, count)
        def _(step):
            copy(
                chunk, step, lax.rem(me - step + count, count), lax.rem(me + step, count)
            ).wait()

        standardize(landed[chunk], plain)

        @pl.loop(0, ROWS)
        def _(row):
            normed = (row_of(plain, row, hidden, span) * gain[...]).astype(jnp.bfloat16)
            inside = mask[pl.ds(chunk * ROWS + row, 1), :]
            projected = jnp.dot(weights[...], normed, preferred_element_type=jnp.float32)
            gated = inside * gate[chunk * ROWS + row] * projected
            put_row(sided, row, channels, span, gated)

        pack(sided, outgoing.at[chunk], span)

        @pl.loop(1, quads)
        def _(step):
            out_copy(chunk, step, quad, lax.rem(quad + step, quads)).start()

        out_keep(chunk).start()

    @pl.loop(0, chunks)
    def _(chunk):
        @pl.loop(1, quads)
        def _(step):
            out_copy(
                chunk, step, lax.rem(quad - step + quads, quads), lax.rem(quad + step, quads)
            ).wait()

        out_keep(chunk).wait()


def shards(pair, pair_mask, input_gain, input_weights, out_gate_weight, hidden_gain, out_weight):
    flat = ("gx", "gz")
    quads = lax.axis_size("gz")
    count = lax.axis_size("gx") * quads
    cores = lax.axis_size("gy")
    local, tall, span = pair.shape
    rows = tall // quads
    chunks = rows // ROWS
    channels = input_gain.shape[0]
    hidden = hidden_gain.shape[0]
    depth = hidden // count
    own_mask = lax.dynamic_slice_in_dim(pair_mask, lax.axis_index("gz") * rows, rows, 0)
    mask_values = own_mask.astype(jnp.float32)
    turned = jnp.concatenate(
        [jnp.swapaxes(input_weights, 1, 2), jnp.swapaxes(out_gate_weight, 0, 1)[None]], axis=0
    )
    wide_gain = jnp.broadcast_to(input_gain[:, None], (channels, span))
    wide_hidden = jnp.broadcast_to(hidden_gain[:, None], (hidden, span))
    near = pl.BlockSpec(memory_space=pltpu.VMEM)
    far = pl.BlockSpec(memory_space=pl.ANY)
    copies = pltpu.SemaphoreType.DMA
    wide_left, far_right, gate = pl.pallas_call(
        functools.partial(front_kernel, flat, count, quads),
        out_shape=(
            jax.ShapeDtypeStruct((depth, count, rows, span * cores), jnp.bfloat16),
            jax.ShapeDtypeStruct((depth, count, rows, span), jnp.bfloat16),
            jax.ShapeDtypeStruct((rows, channels, span), jnp.float32),
        ),
        in_specs=[far, near, near, near],
        out_specs=(far, far, near),
        scratch_shapes=[
            pltpu.VMEM((chunks, channels, ROWS, span), jnp.bfloat16),
            pltpu.VMEM((span // LANES, channels * ROWS, LANES), jnp.float32),
            pltpu.VMEM((2, span // LANES, hidden * ROWS, LANES), jnp.float32),
            pltpu.VMEM((2, chunks, hidden, ROWS, span), jnp.bfloat16),
            copies((chunks, quads)),
            copies((chunks, quads)),
            copies((chunks,)),
            copies((2, chunks, count)),
            copies((2, chunks, count)),
            copies((chunks, cores)),
            copies((chunks, cores)),
            copies((2, chunks)),
        ],
        compiler_params=pltpu.CompilerParams(
            collective_id=0, has_side_effects=True, vmem_limit_bytes=40 << 20
        ),
    )(pair, mask_values, wide_gain, turned)
    return pl.pallas_call(
        functools.partial(back_kernel, flat, count, quads),
        out_shape=jax.ShapeDtypeStruct(pair.shape, jnp.bfloat16),
        in_specs=[near] * 6,
        out_specs=far,
        scratch_shapes=[
            pltpu.VMEM((depth, count, chunks, ROWS, span), jnp.bfloat16),
            pltpu.VMEM((chunks, hidden, ROWS, span), jnp.bfloat16),
            pltpu.VMEM((span // LANES, hidden * ROWS, LANES), jnp.float32),
            pltpu.VMEM((span // LANES, channels * ROWS, LANES), jnp.float32),
            pltpu.VMEM((chunks, channels, ROWS, span), jnp.bfloat16),
            copies((chunks, count)),
            copies((chunks, count)),
            copies((chunks, quads)),
            copies((chunks, quads)),
            copies((chunks,)),
        ],
        compiler_params=pltpu.CompilerParams(
            collective_id=1, has_side_effects=True, vmem_limit_bytes=48 << 20
        ),
    )(
        wide_left.reshape(depth, count * rows, span * cores),
        far_right.reshape(depth, count * rows, span),
        gate,
        mask_values,
        wide_hidden,
        jnp.swapaxes(out_weight, 0, 1),
    )


def solution(mesh):
    placed = (P("gz", "gx", "gy"), P("gx", "gy"), P(), P(), P(), P(), P())
    return jax.shard_map(
        shards, mesh=mesh, in_specs=placed, out_specs=P("gz", "gx", "gy"), check_vma=False
    )
```

```python
import functools

import jax
import jax.numpy as jnp
from jax import lax
from jax.experimental import pallas as pl
from jax.experimental.pallas import tpu as pltpu
from jax.sharding import PartitionSpec as P

EPSILON = 1e-05
MESH = pl.DeviceIdType.MESH


def position(axes):
    at = 0
    for name in axes:
        at = at * lax.axis_size(name) + lax.axis_index(name)
    return at


def coordinates(axes, at):
    where = {}
    for name in reversed(axes):
        where[name] = lax.rem(at, lax.axis_size(name))
        at = at // lax.axis_size(name)
    return where


ROWS = 8
LANES = 128


def panels(span):
    return [(at, slice(at * LANES, (at + 1) * LANES)) for at in range(span // LANES)]


def row_of(store, row, height, span):
    parts = [store[at, pl.ds(row, height, stride=ROWS), :] for at, _ in panels(span)]
    return jnp.concatenate(parts, axis=1)


def put_row(store, row, height, span, value):
    for at, lanes in panels(span):
        store[at, pl.ds(row, height, stride=ROWS), :] = value[:, lanes]


def pack(store, target, span):
    for at, lanes in panels(span):
        height = store.shape[1] // ROWS
        target[:, :, lanes] = store[at].reshape(height, ROWS, LANES).astype(jnp.bfloat16)


def greet(groups):
    barrier = pltpu.get_barrier_semaphore()
    total = 0
    for axes, count in groups:
        me = position(axes)

        @pl.loop(1, count)
        def _(step):
            there = coordinates(axes, lax.rem(me + step, count))
            pl.semaphore_signal(barrier, inc=1, device_id=there, device_id_type=MESH)

        total += count - 1
    pl.semaphore_wait(barrier, total)


def standardize(source, plain):
    values = source.astype(jnp.float32)
    average = jnp.sum(values, axis=0) / values.shape[0]
    centred = values - average
    spread = jnp.sum(centred * centred, axis=0) / values.shape[0]
    result = centred * lax.rsqrt(spread + EPSILON)
    for at, lanes in panels(values.shape[2]):
        plain[at] = result[:, :, lanes].reshape(plain.shape[1:])


def whole_kernel(
    flat, count, quads, pair, mask, input_gain, input_weights, out_gate_weight, hidden_gain, out_weight,
    update,
    turned, spread_gain, wide_left, far_right, gate, triangle,
    landed, plain, sided, outgoing, returned, finished,
    pair_send, pair_recv, pair_own, sends, receives, gsend, greceive, own,
    back_send, back_recv, out_send, out_recv, out_own,
):
    me = position(flat)
    quad = lax.axis_index("gz")
    core = lax.axis_index("gy")
    cores = lax.axis_size("gy")
    chunks, channels, _, span = landed.shape
    local = pair.shape[0]
    rows = chunks * ROWS
    hidden = outgoing.shape[2]
    channels = landed.shape[1]
    depth = hidden // count
    greet(((flat, count), (("gy",), cores)))

    def wide_gain(at):
        return jnp.concatenate([spread_gain[at]] * (span // LANES), axis=1)

    def inside_of(chunk, row):
        first = quad * rows + chunk * ROWS + row
        return mask[pl.ds(first, 1), :].astype(jnp.float32)

    columns = pl.ds(pl.multiple_of(core * span, span), span)

    def pair_copy(chunk, step, sender, target):
        first = pl.multiple_of(target * rows + chunk * ROWS, ROWS)
        return pltpu.make_async_remote_copy(
            src_ref=pair.at[:, pl.ds(first, ROWS), :],
            dst_ref=landed.at[chunk, pl.ds(sender * local, local)],
            send_sem=pair_send.at[chunk, step],
            recv_sem=pair_recv.at[chunk, step],
            device_id={"gz": target},
            device_id_type=MESH,
        )

    def pair_keep(chunk):
        first = pl.multiple_of(quad * rows + chunk * ROWS, ROWS)
        return pltpu.make_async_copy(
            pair.at[:, pl.ds(first, ROWS), :],
            landed.at[chunk, pl.ds(quad * local, local)],
            pair_own.at[chunk],
        )

    def landing(side, chunk, sender):
        cut = pl.ds(pl.multiple_of(chunk * ROWS, ROWS), ROWS)
        if side == 0:
            return wide_left.at[:, sender, cut, columns]
        return far_right.at[:, sender, cut, :]

    def copy(side, chunk, step, sender, target):
        return pltpu.make_async_remote_copy(
            src_ref=outgoing.at[side, chunk, pl.ds(target * depth, depth)],
            dst_ref=landing(side, chunk, sender),
            send_sem=sends.at[side, chunk, step],
            recv_sem=receives.at[side, chunk, step],
            device_id=coordinates(flat, target),
            device_id_type=MESH,
        )

    def keep(side, chunk):
        return pltpu.make_async_copy(
            outgoing.at[side, chunk, pl.ds(me * depth, depth)],
            landing(side, chunk, me),
            own.at[side, chunk],
        )

    def passed(chunk, ahead):
        cut = pl.ds(pl.multiple_of(chunk * ROWS, ROWS), ROWS)
        return pltpu.make_async_remote_copy(
            src_ref=wide_left.at[:, :, cut, columns],
            dst_ref=wide_left.at[:, :, cut, columns],
            send_sem=gsend.at[chunk, ahead],
            recv_sem=greceive.at[chunk, ahead],
            device_id={"gy": lax.rem(core + ahead, cores)},
            device_id_type=MESH,
        )

    @pl.loop(0, chunks)
    def _(chunk):
        pair_keep(chunk).start()

        @pl.loop(1, quads)
        def _(step):
            pair_copy(chunk, step, quad, lax.rem(quad + step, quads)).start()

    for at in range(4):
        turned[at] = input_weights[at].astype(jnp.float32).T.astype(jnp.bfloat16)
    turned[4] = out_gate_weight[...].astype(jnp.float32).T.astype(jnp.bfloat16)
    turned[5] = out_weight[...].astype(jnp.float32).T.astype(jnp.bfloat16)
    spread_gain[0] = jnp.broadcast_to(input_gain[...], (LANES, channels)).T
    spread_gain[1] = jnp.broadcast_to(hidden_gain[...], (LANES, hidden)).T

    @pl.loop(0, chunks)
    def _(chunk):
        @pl.loop(1, quads)
        def _(step):
            pair_copy(
                chunk, step, lax.rem(quad - step + quads, quads), lax.rem(quad + step, quads)
            ).wait()

        pair_keep(chunk).wait()
        standardize(landed[chunk], plain)

        @pl.loop(0, ROWS)
        def _(row):
            normed = (row_of(plain, row, channels, span) * wide_gain(0)).astype(jnp.bfloat16)
            inside = inside_of(chunk, row)

            def product(at):
                return jnp.dot(turned[at], normed, preferred_element_type=jnp.float32)

            for side in range(2):
                gated = inside * jax.nn.sigmoid(product(2 * side)) * product(2 * side + 1)
                put_row(sided.at[side], row, hidden, span, gated)
            gate[chunk * ROWS + row] = jax.nn.sigmoid(product(4))

        for side in range(2):
            pack(sided.at[side], outgoing.at[side, chunk], span)

        for side in range(2):
            @pl.loop(1, count)
            def _(step):
                copy(side, chunk, step, me, lax.rem(me + step, count)).start()

            keep(side, chunk).start()

    @pl.loop(0, chunks)
    def _(chunk):
        for side in range(2):
            @pl.loop(1, count)
            def _(step):
                copy(
                    side, chunk, step, lax.rem(me - step + count, count), lax.rem(me + step, count)
                ).wait()

            keep(side, chunk).wait()
            if side == 0:
                for ahead in range(1, cores):
                    passed(chunk, ahead).start()

    @pl.loop(0, chunks)
    def _(chunk):
        for ahead in range(1, cores):
            passed(chunk, ahead).wait()

    def back_copy(chunk, step, sender, target):
        return pltpu.make_async_remote_copy(
            src_ref=triangle.at[:, target, chunk],
            dst_ref=returned.at[chunk, pl.ds(sender * depth, depth)],
            send_sem=back_send.at[chunk, step],
            recv_sem=back_recv.at[chunk, step],
            device_id=coordinates(flat, target),
            device_id_type=MESH,
        )

    def out_copy(chunk, step, sender, target):
        first = pl.multiple_of(sender * rows + chunk * ROWS, ROWS)
        return pltpu.make_async_remote_copy(
            src_ref=finished.at[chunk, pl.ds(target * local, local)],
            dst_ref=update.at[:, pl.ds(first, ROWS), :],
            send_sem=out_send.at[chunk, step],
            recv_sem=out_recv.at[chunk, step],
            device_id={"gz": target},
            device_id_type=MESH,
        )

    def out_keep(chunk):
        first = pl.multiple_of(quad * rows + chunk * ROWS, ROWS)
        return pltpu.make_async_copy(
            finished.at[chunk, pl.ds(quad * local, local)],
            update.at[:, pl.ds(first, ROWS), :],
            out_own.at[chunk],
        )

    @pl.loop(0, depth)
    def _(at):
        product = lax.dot_general(
            wide_left[at].reshape(count * rows, -1),
            far_right[at].reshape(count * rows, -1), (((0,), (0,)), ((), ())),
            preferred_element_type=jnp.float32,
        )
        triangle[at] = product.reshape(count, chunks, ROWS, span).astype(jnp.bfloat16)

    @pl.loop(0, chunks)
    def _(chunk):
        @pl.loop(1, count)
        def _(step):
            back_copy(chunk, step, me, lax.rem(me + step, count)).start()

    @pl.loop(0, chunks)
    def _(chunk):
        @pl.loop(0, depth)
        def _(at):
            returned[chunk, me * depth + at] = triangle[at, me, chunk]

        @pl.loop(1, count)
        def _(step):
            back_copy(
                chunk, step, lax.rem(me - step + count, count), lax.rem(me + step, count)
            ).wait()

        standardize(returned[chunk], plain)

        @pl.loop(0, ROWS)
        def _(row):
            normed = (row_of(plain, row, hidden, span) * wide_gain(1)).astype(jnp.bfloat16)
            inside = inside_of(chunk, row)
            projected = jnp.dot(turned[5], normed, preferred_element_type=jnp.float32)
            gated = inside * gate[chunk * ROWS + row] * projected
            put_row(sided.at[0], row, channels, span, gated)

        pack(sided.at[0], finished.at[chunk], span)

        @pl.loop(1, quads)
        def _(step):
            out_copy(chunk, step, quad, lax.rem(quad + step, quads)).start()

        out_keep(chunk).start()

    @pl.loop(0, chunks)
    def _(chunk):
        @pl.loop(1, quads)
        def _(step):
            out_copy(
                chunk, step, lax.rem(quad - step + quads, quads), lax.rem(quad + step, quads)
            ).wait()

        out_keep(chunk).wait()


def shards(pair, pair_mask, input_gain, input_weights, out_gate_weight, hidden_gain, out_weight):
    flat = ("gx", "gz")
    quads = lax.axis_size("gz")
    count = lax.axis_size("gx") * quads
    cores = lax.axis_size("gy")
    local, tall, span = pair.shape
    rows = tall // quads
    chunks = rows // ROWS
    channels = input_gain.shape[0]
    hidden = hidden_gain.shape[0]
    depth = hidden // count
    near = pl.BlockSpec(memory_space=pltpu.VMEM)
    far = pl.BlockSpec(memory_space=pl.ANY)
    copies = pltpu.SemaphoreType.DMA
    tiles = span // LANES
    tallest = max(channels, hidden)
    return pl.pallas_call(
        functools.partial(whole_kernel, flat, count, quads),
        out_shape=jax.ShapeDtypeStruct(pair.shape, jnp.bfloat16),
        in_specs=[far] + [near] * 6,
        out_specs=far,
        scratch_shapes=[
            pltpu.VMEM((6, tallest, tallest), jnp.bfloat16),
            pltpu.VMEM((2, tallest, LANES), jnp.float32),
            pltpu.VMEM((depth, count, rows, span * cores), jnp.bfloat16),
            pltpu.VMEM((depth, count, rows, span), jnp.bfloat16),
            pltpu.VMEM((rows, channels, span), jnp.float32),
            pltpu.VMEM((depth, count, chunks, ROWS, span), jnp.bfloat16),
            pltpu.VMEM((chunks, channels, ROWS, span), jnp.bfloat16),
            pltpu.VMEM((tiles, tallest * ROWS, LANES), jnp.float32),
            pltpu.VMEM((2, tiles, tallest * ROWS, LANES), jnp.float32),
            pltpu.VMEM((2, chunks, hidden, ROWS, span), jnp.bfloat16),
            pltpu.VMEM((chunks, hidden, ROWS, span), jnp.bfloat16),
            pltpu.VMEM((chunks, channels, ROWS, span), jnp.bfloat16),
            copies((chunks, quads)),
            copies((chunks, quads)),
            copies((chunks,)),
            copies((2, chunks, count)),
            copies((2, chunks, count)),
            copies((chunks, cores)),
            copies((chunks, cores)),
            copies((2, chunks)),
            copies((chunks, count)),
            copies((chunks, count)),
            copies((chunks, quads)),
            copies((chunks, quads)),
            copies((chunks,)),
        ],
        compiler_params=pltpu.CompilerParams(
            collective_id=0, has_side_effects=True, vmem_limit_bytes=60 << 20
        ),
    )(
        pair,
        pair_mask,
        input_gain[None],
        input_weights,
        out_gate_weight,
        hidden_gain[None],
        out_weight,
    )


def solution(mesh):
    placed = (P("gz", "gx", "gy"), P("gx", "gy"), P(), P(), P(), P(), P())
    return jax.shard_map(
        shards, mesh=mesh, in_specs=placed, out_specs=P("gz", "gx", "gy"), check_vma=False
    )
```

```python
import functools

import jax
import jax.numpy as jnp
from jax import lax
from jax.experimental import pallas as pl
from jax.experimental.pallas import tpu as pltpu
from jax.sharding import PartitionSpec as P

EPSILON = 1e-05
MESH = pl.DeviceIdType.MESH


def position(axes):
    at = 0
    for name in axes:
        at = at * lax.axis_size(name) + lax.axis_index(name)
    return at


def coordinates(axes, at):
    where = {}
    for name in reversed(axes):
        where[name] = lax.rem(at, lax.axis_size(name))
        at = at // lax.axis_size(name)
    return where


ROWS = 8
LANES = 128


def panels(span):
    return [(at, slice(at * LANES, (at + 1) * LANES)) for at in range(span // LANES)]


def row_of(store, row, height, span):
    parts = [store[at, pl.ds(row, height, stride=ROWS), :] for at, _ in panels(span)]
    return jnp.concatenate(parts, axis=1)


def put_row(store, row, height, span, value):
    for at, lanes in panels(span):
        store[at, pl.ds(row, height, stride=ROWS), :] = value[:, lanes]


def pack(store, target, span):
    for at, lanes in panels(span):
        height = store.shape[1] // ROWS
        target[:, :, lanes] = store[at].reshape(height, ROWS, LANES).astype(jnp.bfloat16)


def greet(groups):
    barrier = pltpu.get_barrier_semaphore()
    total = 0
    for axes, count in groups:
        me = position(axes)

        @pl.loop(1, count)
        def _(step):
            there = coordinates(axes, lax.rem(me + step, count))
            pl.semaphore_signal(barrier, inc=1, device_id=there, device_id_type=MESH)

        total += count - 1
    pl.semaphore_wait(barrier, total)


def standardize(source, plain):
    values = source.astype(jnp.float32)
    average = jnp.sum(values, axis=0) / values.shape[0]
    centred = values - average
    spread = jnp.sum(centred * centred, axis=0) / values.shape[0]
    result = centred * lax.rsqrt(spread + EPSILON)
    for at, lanes in panels(values.shape[2]):
        plain[at] = result[:, :, lanes].reshape(plain.shape[1:])


def whole_kernel(
    flat, count, quads, pair, mask, input_gain, input_weights, out_gate_weight, hidden_gain, out_weight,
    update,
    turned, spread_gain, wide_left, far_right, gate, triangle,
    landed, plain, sided, outgoing, returned, finished,
    pair_send, pair_recv, pair_own, sends, receives, gsend, greceive, own,
    back_send, back_recv, out_send, out_recv, out_own,
):
    me = position(flat)
    quad = lax.axis_index("gz")
    core = lax.axis_index("gy")
    cores = lax.axis_size("gy")
    chunks, channels, _, span = landed.shape
    local = pair.shape[0]
    rows = chunks * ROWS
    hidden = outgoing.shape[2]
    channels = landed.shape[1]
    depth = hidden // count
    greet(((flat, count), (("gy",), cores)))

    def wide_gain(at):
        return jnp.concatenate([spread_gain[at]] * (span // LANES), axis=1)

    def inside_of(chunk, row):
        first = quad * rows + chunk * ROWS + row
        return mask[pl.ds(first, 1), :].astype(jnp.float32)

    columns = pl.ds(pl.multiple_of(core * span, span), span)

    def pair_copy(chunk, step, sender, target):
        first = pl.multiple_of(target * rows + chunk * ROWS, ROWS)
        return pltpu.make_async_remote_copy(
            src_ref=pair.at[:, pl.ds(first, ROWS), :],
            dst_ref=landed.at[chunk, pl.ds(sender * local, local)],
            send_sem=pair_send.at[chunk, step],
            recv_sem=pair_recv.at[chunk, step],
            device_id={"gz": target},
            device_id_type=MESH,
        )

    def pair_keep(chunk):
        first = pl.multiple_of(quad * rows + chunk * ROWS, ROWS)
        return pltpu.make_async_copy(
            pair.at[:, pl.ds(first, ROWS), :],
            landed.at[chunk, pl.ds(quad * local, local)],
            pair_own.at[chunk],
        )

    def landing(side, chunk, sender):
        cut = pl.ds(pl.multiple_of(chunk * ROWS, ROWS), ROWS)
        if side == 0:
            return wide_left.at[:, sender, cut, columns]
        return far_right.at[:, sender, cut, :]

    def copy(side, chunk, step, sender, target):
        return pltpu.make_async_remote_copy(
            src_ref=outgoing.at[side, chunk, pl.ds(target * depth, depth)],
            dst_ref=landing(side, chunk, sender),
            send_sem=sends.at[side, chunk, step],
            recv_sem=receives.at[side, chunk, step],
            device_id=coordinates(flat, target),
            device_id_type=MESH,
        )

    def keep(side, chunk):
        return pltpu.make_async_copy(
            outgoing.at[side, chunk, pl.ds(me * depth, depth)],
            landing(side, chunk, me),
            own.at[side, chunk],
        )

    def passed(chunk, ahead):
        cut = pl.ds(pl.multiple_of(chunk * ROWS, ROWS), ROWS)
        return pltpu.make_async_remote_copy(
            src_ref=wide_left.at[:, :, cut, columns],
            dst_ref=wide_left.at[:, :, cut, columns],
            send_sem=gsend.at[chunk, ahead],
            recv_sem=greceive.at[chunk, ahead],
            device_id={"gy": lax.rem(core + ahead, cores)},
            device_id_type=MESH,
        )

    @pl.loop(0, chunks)
    def _(chunk):
        pair_keep(chunk).start()

        @pl.loop(1, quads)
        def _(step):
            pair_copy(chunk, step, quad, lax.rem(quad + step, quads)).start()

    for at in range(4):
        turned[at] = input_weights[at].astype(jnp.float32).T.astype(jnp.bfloat16)
    turned[4] = out_gate_weight[...].astype(jnp.float32).T.astype(jnp.bfloat16)
    turned[5] = out_weight[...].astype(jnp.float32).T.astype(jnp.bfloat16)
    spread_gain[0] = jnp.broadcast_to(input_gain[...], (LANES, channels)).T
    spread_gain[1] = jnp.broadcast_to(hidden_gain[...], (LANES, hidden)).T

    @pl.loop(0, chunks)
    def _(chunk):
        @pl.loop(1, quads)
        def _(step):
            pair_copy(
                chunk, step, lax.rem(quad - step + quads, quads), lax.rem(quad + step, quads)
            ).wait()

        pair_keep(chunk).wait()
        standardize(landed[chunk], plain)

        def normed_row(row):
            return (row_of(plain, row, channels, span) * wide_gain(0)).astype(jnp.bfloat16)

        def product(at, normed):
            return jnp.dot(turned[at], normed, preferred_element_type=jnp.float32)

        for side in range(2):
            @pl.loop(0, ROWS)
            def _(row):
                normed = normed_row(row)
                gating = inside_of(chunk, row) * jax.nn.sigmoid(product(2 * side, normed))
                put_row(sided.at[side], row, hidden, span, gating * product(2 * side + 1, normed))

            pack(sided.at[side], outgoing.at[side, chunk], span)

            @pl.loop(1, count)
            def _(step):
                copy(side, chunk, step, me, lax.rem(me + step, count)).start()

            keep(side, chunk).start()

        @pl.loop(0, ROWS)
        def _(row):
            gate[chunk * ROWS + row] = jax.nn.sigmoid(product(4, normed_row(row)))

    @pl.loop(0, chunks)
    def _(chunk):
        for side in range(2):
            @pl.loop(1, count)
            def _(step):
                copy(
                    side, chunk, step, lax.rem(me - step + count, count), lax.rem(me + step, count)
                ).wait()

            keep(side, chunk).wait()
            if side == 0:
                for ahead in range(1, cores):
                    passed(chunk, ahead).start()

    @pl.loop(0, chunks)
    def _(chunk):
        for ahead in range(1, cores):
            passed(chunk, ahead).wait()

    def back_copy(chunk, step, sender, target):
        return pltpu.make_async_remote_copy(
            src_ref=triangle.at[:, target, chunk],
            dst_ref=returned.at[chunk, pl.ds(sender * depth, depth)],
            send_sem=back_send.at[chunk, step],
            recv_sem=back_recv.at[chunk, step],
            device_id=coordinates(flat, target),
            device_id_type=MESH,
        )

    def out_copy(chunk, step, sender, target):
        first = pl.multiple_of(sender * rows + chunk * ROWS, ROWS)
        return pltpu.make_async_remote_copy(
            src_ref=finished.at[chunk, pl.ds(target * local, local)],
            dst_ref=update.at[:, pl.ds(first, ROWS), :],
            send_sem=out_send.at[chunk, step],
            recv_sem=out_recv.at[chunk, step],
            device_id={"gz": target},
            device_id_type=MESH,
        )

    def out_keep(chunk):
        first = pl.multiple_of(quad * rows + chunk * ROWS, ROWS)
        return pltpu.make_async_copy(
            finished.at[chunk, pl.ds(quad * local, local)],
            update.at[:, pl.ds(first, ROWS), :],
            out_own.at[chunk],
        )

    @pl.loop(0, depth)
    def _(at):
        product = lax.dot_general(
            wide_left[at].reshape(count * rows, -1),
            far_right[at].reshape(count * rows, -1), (((0,), (0,)), ((), ())),
            preferred_element_type=jnp.float32,
        )
        triangle[at] = product.reshape(count, chunks, ROWS, span).astype(jnp.bfloat16)

    @pl.loop(0, chunks)
    def _(chunk):
        @pl.loop(1, count)
        def _(step):
            back_copy(chunk, step, me, lax.rem(me + step, count)).start()

    @pl.loop(0, chunks)
    def _(chunk):
        @pl.loop(0, depth)
        def _(at):
            returned[chunk, me * depth + at] = triangle[at, me, chunk]

        @pl.loop(1, count)
        def _(step):
            back_copy(
                chunk, step, lax.rem(me - step + count, count), lax.rem(me + step, count)
            ).wait()

        standardize(returned[chunk], plain)

        @pl.loop(0, ROWS)
        def _(row):
            normed = (row_of(plain, row, hidden, span) * wide_gain(1)).astype(jnp.bfloat16)
            inside = inside_of(chunk, row)
            projected = jnp.dot(turned[5], normed, preferred_element_type=jnp.float32)
            gated = inside * gate[chunk * ROWS + row] * projected
            put_row(sided.at[0], row, channels, span, gated)

        pack(sided.at[0], finished.at[chunk], span)

        @pl.loop(1, quads)
        def _(step):
            out_copy(chunk, step, quad, lax.rem(quad + step, quads)).start()

        out_keep(chunk).start()

    @pl.loop(0, chunks)
    def _(chunk):
        @pl.loop(1, quads)
        def _(step):
            out_copy(
                chunk, step, lax.rem(quad - step + quads, quads), lax.rem(quad + step, quads)
            ).wait()

        out_keep(chunk).wait()


def shards(pair, pair_mask, input_gain, input_weights, out_gate_weight, hidden_gain, out_weight):
    flat = ("gx", "gz")
    quads = lax.axis_size("gz")
    count = lax.axis_size("gx") * quads
    cores = lax.axis_size("gy")
    local, tall, span = pair.shape
    rows = tall // quads
    chunks = rows // ROWS
    channels = input_gain.shape[0]
    hidden = hidden_gain.shape[0]
    depth = hidden // count
    near = pl.BlockSpec(memory_space=pltpu.VMEM)
    far = pl.BlockSpec(memory_space=pl.ANY)
    copies = pltpu.SemaphoreType.DMA
    tiles = span // LANES
    tallest = max(channels, hidden)
    return pl.pallas_call(
        functools.partial(whole_kernel, flat, count, quads),
        out_shape=jax.ShapeDtypeStruct(pair.shape, jnp.bfloat16),
        in_specs=[far] + [near] * 6,
        out_specs=far,
        scratch_shapes=[
            pltpu.VMEM((6, tallest, tallest), jnp.bfloat16),
            pltpu.VMEM((2, tallest, LANES), jnp.float32),
            pltpu.VMEM((depth, count, rows, span * cores), jnp.bfloat16),
            pltpu.VMEM((depth, count, rows, span), jnp.bfloat16),
            pltpu.VMEM((rows, channels, span), jnp.float32),
            pltpu.VMEM((depth, count, chunks, ROWS, span), jnp.bfloat16),
            pltpu.VMEM((chunks, channels, ROWS, span), jnp.bfloat16),
            pltpu.VMEM((tiles, tallest * ROWS, LANES), jnp.float32),
            pltpu.VMEM((2, tiles, tallest * ROWS, LANES), jnp.float32),
            pltpu.VMEM((2, chunks, hidden, ROWS, span), jnp.bfloat16),
            pltpu.VMEM((chunks, hidden, ROWS, span), jnp.bfloat16),
            pltpu.VMEM((chunks, channels, ROWS, span), jnp.bfloat16),
            copies((chunks, quads)),
            copies((chunks, quads)),
            copies((chunks,)),
            copies((2, chunks, count)),
            copies((2, chunks, count)),
            copies((chunks, cores)),
            copies((chunks, cores)),
            copies((2, chunks)),
            copies((chunks, count)),
            copies((chunks, count)),
            copies((chunks, quads)),
            copies((chunks, quads)),
            copies((chunks,)),
        ],
        compiler_params=pltpu.CompilerParams(
            collective_id=0, has_side_effects=True, vmem_limit_bytes=60 << 20
        ),
    )(
        pair,
        pair_mask,
        input_gain[None],
        input_weights,
        out_gate_weight,
        hidden_gain[None],
        out_weight,
    )


def solution(mesh):
    placed = (P("gz", "gx", "gy"), P("gx", "gy"), P(), P(), P(), P(), P())
    return jax.shard_map(
        shards, mesh=mesh, in_specs=placed, out_specs=P("gz", "gx", "gy"), check_vma=False
    )
```
